32 devices in a mesh: row: 8 (over z, x), col: 4 (over y, core).
Axes of the slice: x: 2, y: 2, z: 4, core: 2. Of those that a mesh axis runs over, the one named last changes fastest.
Arguments:
- trailing: float32 [16384, 8192], P('row', 'col'), may hold values from -6 to 6
- vectors: float32 [16384, 256], P(('row', 'col')), may hold values from -0.1875 to 0.1875
- tfactor: float32 [256, 256], replicated, may hold values from -0.375 to 0.375
Outputs:
- updated: float32 [16384, 8192], P('row', 'col')
The draws below stay inside these ranges and needn't reach their ends.
All inputs are finite; a program needn't handle non-finite values.
Results may differ from the reference program's by a relative error of at most 0.0003.
Values sent between devices are 32-bit elements.
A program may use at most 128 MiB of HBM per device.

```python
import jax
import jax.numpy as jnp
from jax import lax

N = 8192
K = 256
M = 16384


def steps_of(own_key, shape, shards, smallest, high):
    loudness, own = 1.0, jax.random.fold_in(own_key, 6)
    for axis_at, shards_of in shards:
        heights = jnp.exp(jax.random.uniform(jax.random.fold_in(own, axis_at), (shards_of,), jnp.float32, smallest / len(shards), high / len(shards)))
        loudness = loudness * jnp.repeat(heights, shape[axis_at] // shards_of).reshape([-1 if axis == axis_at else 1 for axis in range(len(shape))])
    return loudness


def gaussian(own_key, dims, width, most, split=(), kind=jnp.bfloat16):
    loudness = steps_of(own_key, dims, split, -0.22, 0.18) if split else 1.0
    drawn = jax.random.normal(own_key, dims, jnp.float32) * width * loudness
    return jnp.minimum(jnp.maximum(drawn, -most), most).astype(kind)


def setup_inputs(seed: int = 0) -> dict:
    arg_keys = jax.random.split(jax.random.key(seed), 4)
    return {
        "trailing": gaussian(arg_keys[0], (M, N), 1.0, 6.0, ((0, 8), (1, 4)), jnp.float32),
        "vectors": gaussian(arg_keys[1], (M, K), (M // 16) ** -0.5, 0.1875, ((0, 32),), jnp.float32),
        "tfactor": gaussian(arg_keys[2], (K, K), K ** -0.5, 0.375, (), jnp.float32),
    }


def reference(trailing, vectors, tfactor):
    high = lax.Precision.HIGHEST
    coeffs = jnp.dot(vectors.T, trailing, precision=high, preferred_element_type=jnp.float32)
    scaled = jnp.dot(tfactor, coeffs, precision=high, preferred_element_type=jnp.float32)
    return trailing - jnp.dot(vectors, scaled, precision=high, preferred_element_type=jnp.float32)
```

```python
import functools

import jax
import jax.numpy as jnp
from jax import lax
from jax.experimental import pallas as pl
from jax.experimental.pallas import tpu as pltpu
from jax.sharding import PartitionSpec as P

MESH = pl.DeviceIdType.MESH
F32, BF16 = jnp.float32, jnp.bfloat16
PIECES = 4
QUARTERS = 4


def split(x):
    high = x.astype(BF16)
    return high, (x - high.astype(F32)).astype(BF16)


def dot3(a_high, a_low, b_high, b_low):
    dot = functools.partial(jnp.dot, preferred_element_type=F32)
    return dot(a_high, b_high) + (dot(a_low, b_high) + dot(a_high, b_low))


def sum_kernel(
    ring, c_hbm, v_ref, t_ref, c_ref, near, scaled,
    acc, vt_high, vt_low, got, c_sem,
    sib_send, sib_recv, y_send, y_recv, f_send, f_recv, r_send, r_recv, g_send, g_recv,
):
    row, col = lax.axis_index("row"), lax.axis_index("col")
    core, y = lax.rem(col, 2), lax.div(col, 2)
    sibling = y * 2 + (1 - core)
    across = (1 - y) * 2 + core
    across_sibling = (1 - y) * 2 + (1 - core)
    half = ring // 2
    z, x = lax.div(row, 2), lax.rem(row, 2)
    at = jnp.where(x == 0, z, ring - 1 - z)

    def row_of(place):
        return jnp.where(place < half, 2 * place, 2 * (ring - 1 - place) + 1)

    def wrap(i):
        return lax.rem(i + 2 * ring, ring)

    hops = (row_of(wrap(at + 1)), row_of(wrap(at - 1)))
    own, depth = v_ref.shape
    width = c_ref.shape[2]

    def place_of(i):
        step = lax.div(i, 2) + 1
        return wrap(jnp.where(lax.rem(i, 2) == 0, at - step, at + step)) if not isinstance(i, int) else wrap(
            at - (i // 2 + 1) if i % 2 == 0 else at + (i // 2 + 1))

    def chunk_of(i):
        return jnp.where(i == ring - 1, at, place_of(i))

    def c_copy(chunk):
        return pltpu.make_async_copy(
            c_hbm.at[:, pl.ds(pl.multiple_of(chunk * width, width), width)], c_ref.at[chunk], c_sem.at[chunk]
        )

    def load(i, carry):
        c_copy(chunk_of(i)).start()
        return carry

    lax.fori_loop(0, ring, load, 0)

    barrier = pltpu.get_barrier_semaphore()
    friends = [(row, sibling), (row, across), (hops[0], col), (hops[1], col)]
    for friend in friends:
        pl.semaphore_signal(barrier, inc=1, device_id=friend, device_id_type=MESH)
    pl.semaphore_wait(barrier, len(friends))

    def remote(src, dst, send, recv, to):
        return pltpu.make_async_remote_copy(
            src_ref=src, dst_ref=dst, send_sem=send, recv_sem=recv, device_id=to, device_id_type=MESH
        )

    size = own // PIECES
    y_copies = []
    for q in range(PIECES):
        rows = pl.ds(q * size, size)
        copy = remote(v_ref.at[rows], near.at[col, rows], y_send.at[q], y_recv.at[q], (row, across))
        copy.start()
        y_copies.append(copy)
    sib = remote(v_ref, near.at[col], sib_send, sib_recv, (row, sibling))
    sib.start()

    def keep(block, first, count):
        rows = pl.ds(first, count)
        high, low = split(near[block, rows].T)
        vt_high[block, :, rows] = high
        vt_low[block, :, rows] = low

    near[col] = v_ref[...]
    keep(col, 0, own)

    def product(chunk, block, first, count):
        rows = pl.ds(pl.multiple_of(block * own + first, size), count)
        high, low = split(c_ref[chunk, rows])
        part = pl.ds(first, count)
        return dot3(vt_high[block, :, part], vt_low[block, :, part], high, low)

    sib.wait()
    keep(sibling, 0, own)

    def begin(i, carry):
        chunk = chunk_of(i)
        c_copy(chunk).wait()
        acc[chunk] = product(chunk, col, 0, own) + product(chunk, sibling, 0, own)
        return carry

    lax.fori_loop(0, ring, begin, 0)

    def arrive(q):
        rows = pl.ds(q * size, size)
        y_copies[q].wait()
        forward = remote(near.at[across, rows], near.at[across, rows], f_send.at[q], f_recv.at[q], (row, sibling))
        forward.start()
        keep(across, q * size, size)
        forward.wait()
        keep(across_sibling, q * size, size)

    def add(i, q):
        chunk = chunk_of(i)
        acc[chunk] += product(chunk, across, q * size, size) + product(chunk, across_sibling, q * size, size)

    for q in range(PIECES - 1):
        arrive(q)

        def more(i, carry):
            add(i, q)
            return carry

        lax.fori_loop(0, ring, more, 0)
    last = PIECES - 1
    arrive(last)
    part = depth // (2 * QUARTERS)

    def rows_of(way, q):
        return pl.ds((way * QUARTERS + q) * part, part)

    def sum_send(way, step, q, src):
        rows = rows_of(way, q)
        return remote(src.at[rows], got.at[step, rows], r_send.at[way, step, q], r_recv.at[way, step, q], (hops[way], col))

    def finish(i, carry):
        add(i, last)
        return carry

    lax.fori_loop(0, 2, finish, 0)
    for q in range(QUARTERS):
        for way in range(2):
            sum_send(way, 0, q, acc.at[chunk_of(way)]).start()
    lax.fori_loop(2, ring, finish, 0)

    steps = ring - 1

    def reduce(step, carry):
        for q in range(QUARTERS):
            for way in range(2):
                rows = rows_of(way, q)
                chunk = wrap(at - 2 - step) if way == 0 else wrap(at + 2 + step)
                sum_send(way, step, q, got.at[step]).wait_recv()
                got[step, rows] += acc[chunk, rows]

                @pl.when(step < steps - 1)
                def _():
                    sum_send(way, step + 1, q, got.at[step]).start()

        return carry

    lax.fori_loop(0, steps, reduce, 0)

    t_high, t_low = split(t_ref[...])
    high, low = split(got[steps - 1])
    scaled[at] = dot3(t_high, t_low, high, low)

    def gather_send(way, step, q, chunk):
        rows = rows_of(way, q)
        ref = scaled.at[chunk, rows]
        return remote(ref, ref, g_send.at[way, step, q], g_recv.at[way, step, q], (hops[way], col))

    for q in range(QUARTERS):
        for way in range(2):
            gather_send(way, 0, q, at).start()

    def gather(step, carry):
        for q in range(QUARTERS):
            for way in range(2):
                chunk = wrap(at - 1 - step) if way == 0 else wrap(at + 1 + step)
                gather_send(way, step, q, chunk).wait_recv()

                @pl.when(step < steps - 1)
                def _():
                    gather_send(way, step + 1, q, chunk).start()

        return carry

    lax.fori_loop(0, steps, gather, 0)

    def sent(step, carry):
        for q in range(QUARTERS):
            for way in range(2):
                sum_send(way, step, q, got.at[step]).wait_send()
                gather_send(way, step, q, at).wait_send()
        return carry

    lax.fori_loop(0, steps, sent, 0)


def update_kernel(c_ref, near, scaled, out_hbm, v_high, v_low, stage, sem):
    ring, height, width = c_ref.shape
    blocks, own, _ = near.shape
    for b in range(blocks):
        v_high[pl.ds(b * own, own)], v_low[pl.ds(b * own, own)] = split(near[b])
    slots = stage.shape[0]

    def out_copy(chunk, slot):
        return pltpu.make_async_copy(
            stage.at[slot], out_hbm.at[:, pl.ds(pl.multiple_of(chunk * width, width), width)], sem.at[slot]
        )

    def step(chunk, carry):
        slot = lax.rem(chunk, slots)

        @pl.when(chunk >= slots)
        def _():
            out_copy(chunk - slots, slot).wait()

        high, low = split(scaled[chunk])
        for b in range(blocks):
            rows = pl.ds(b * own, own)
            stage[slot, rows] = c_ref[chunk, rows] - dot3(v_high[rows], v_low[rows], high, low)
        out_copy(chunk, slot).start()
        return carry

    lax.fori_loop(0, ring, step, 0)
    for i in range(slots):
        chunk = ring - slots + i
        out_copy(chunk, chunk % slots).wait()


def ring_shards(ring, trailing, vectors, tfactor):
    height, columns = trailing.shape
    own, depth = vectors.shape
    width = columns // ring
    blocks = height // own
    steps = ring - 1
    dma = pltpu.SemaphoreType.DMA
    vmem = pl.BlockSpec(memory_space=pltpu.VMEM)
    hbm = pl.BlockSpec(memory_space=pl.ANY)
    held, near, scaled = pl.pallas_call(
        functools.partial(sum_kernel, ring),
        out_shape=(
            pltpu.VMEM((ring, height, width), F32),
            pltpu.VMEM((blocks, own, depth), F32),
            pltpu.VMEM((ring, depth, width), F32),
        ),
        in_specs=[hbm, vmem, vmem],
        out_specs=(vmem, vmem, vmem),
        scratch_shapes=[
            pltpu.VMEM((ring, depth, width), F32),
            pltpu.VMEM((blocks, depth, own), BF16),
            pltpu.VMEM((blocks, depth, own), BF16),
            pltpu.VMEM((steps, depth, width), F32),
            dma((ring,)),
            dma, dma,
            dma((PIECES,)), dma((PIECES,)), dma((PIECES,)), dma((PIECES,)),
            dma((2, steps, QUARTERS)), dma((2, steps, QUARTERS)),
            dma((2, steps, QUARTERS)), dma((2, steps, QUARTERS)),
        ],
        compiler_params=pltpu.CompilerParams(
            collective_id=0, has_side_effects=True, vmem_limit_bytes=20 << 20
        ),
    )(trailing, vectors, tfactor)
    slots = min(4, ring)
    return pl.pallas_call(
        update_kernel,
        out_shape=jax.ShapeDtypeStruct((height, columns), F32),
        in_specs=[vmem, vmem, vmem],
        out_specs=hbm,
        scratch_shapes=[
            pltpu.VMEM((height, depth), BF16),
            pltpu.VMEM((height, depth), BF16),
            pltpu.VMEM((slots, height, width), F32),
            dma((slots,)),
        ],
        compiler_params=pltpu.CompilerParams(vmem_limit_bytes=20 << 20),
    )(held, near, scaled)


def plain_shards(trailing, vectors, tfactor):
    dot = functools.partial(jnp.dot, precision=lax.Precision.HIGH, preferred_element_type=F32)
    near_vectors = lax.all_gather(vectors, "col", axis=0, tiled=True)
    summed = lax.psum(dot(near_vectors.T, trailing), "row")
    return trailing - dot(near_vectors, dot(tfactor, summed))


def solution(mesh):
    ring, columns = mesh.shape["row"], mesh.shape["col"]
    placed = (P("row", "col"), P(("row", "col"), None), P())

    def shards(trailing, vectors, tfactor):
        width = trailing.shape[1] // ring
        if columns == 4 and ring % 2 == 0 and ring > 2 and width % 128 == 0:
            return ring_shards(ring, trailing, vectors, tfactor)
        return plain_shards(trailing, vectors, tfactor)

    return jax.shard_map(
        shards, mesh=mesh, in_specs=placed, out_specs=P("row", "col"), check_vma=False
    )
```

```python
import functools

import jax
import jax.numpy as jnp
from jax import lax
from jax.experimental import pallas as pl
from jax.experimental.pallas import tpu as pltpu
from jax.sharding import PartitionSpec as P

MESH = pl.DeviceIdType.MESH
F32, BF16 = jnp.float32, jnp.bfloat16
HALVES = 2
PIECES = 2
QUARTERS = 2
G_QUARTERS = 4
LAG = 3


def split(x):
    high = x.astype(BF16)
    return high, (x - high.astype(F32)).astype(BF16)


def dot3(a_high, a_low, b_high, b_low):
    dot = functools.partial(jnp.dot, preferred_element_type=F32)
    return dot(a_high, b_high) + (dot(a_low, b_high) + dot(a_high, b_low))


def sum_kernel(
    ring, c_hbm, v_hbm, t_hbm, c_ref, near, scaled,
    acc, vt, got, t_ref, c_sem, l_sem,
    sib_send, sib_recv, y_send, y_recv, f_send, f_recv, r_send, r_recv, g_send, g_recv,
):
    row, col = lax.axis_index("row"), lax.axis_index("col")
    core, y = lax.rem(col, 2), lax.div(col, 2)
    sibling = y * 2 + (1 - core)
    across = (1 - y) * 2 + core
    across_sibling = (1 - y) * 2 + (1 - core)
    half = ring // 2
    z, x = lax.div(row, 2), lax.rem(row, 2)
    at = jnp.where(x == 0, z, ring - 1 - z)

    def row_of(place):
        return jnp.where(place < half, 2 * place, 2 * (ring - 1 - place) + 1)

    def wrap(i):
        return lax.rem(i + 2 * ring, ring)

    hops = (row_of(wrap(at + 1)), row_of(wrap(at - 1)))
    blocks, own, depth = near.shape
    width = c_ref.shape[2]
    part_depth = depth // HALVES
    steps = ring - 1

    def chunk_of(i):
        step = lax.div(i, 2) + 1
        return jnp.where(i == ring - 1, at, wrap(jnp.where(lax.rem(i, 2) == 0, at - step, at + step)))

    def c_copy(chunk):
        return pltpu.make_async_copy(
            c_hbm.at[:, pl.ds(pl.multiple_of(chunk * width, width), width)], c_ref.at[chunk], c_sem.at[chunk]
        )

    v_copy = pltpu.make_async_copy(v_hbm, near.at[col], l_sem.at[0])
    t_copy = pltpu.make_async_copy(t_hbm, t_ref, l_sem.at[1])
    v_copy.start()

    barrier = pltpu.get_barrier_semaphore()
    friends = [(row, sibling), (row, across), (hops[0], col), (hops[1], col)]
    for friend in friends:
        pl.semaphore_signal(barrier, inc=1, device_id=friend, device_id_type=MESH)
    pl.semaphore_wait(barrier, len(friends))

    def remote(src, dst, send, recv, to):
        return pltpu.make_async_remote_copy(
            src_ref=src, dst_ref=dst, send_sem=send, recv_sem=recv, device_id=to, device_id_type=MESH
        )

    size = own // PIECES

    def y_copy(h, q):
        there = (pl.ds(q * size, size), pl.ds(h * part_depth, part_depth))
        return remote(v_hbm.at[there], near.at[(col,) + there], y_send.at[h, q], y_recv.at[h, q], (row, across))

    def forward(h, q):
        there = (across, pl.ds(q * size, size), pl.ds(h * part_depth, part_depth))
        return remote(near.at[there], near.at[there], f_send.at[h, q], f_recv.at[h, q], (row, sibling))

    for h in range(HALVES):
        for q in range(PIECES):
            y_copy(h, q).start()
    sib = remote(v_hbm, near.at[col], sib_send, sib_recv, (row, sibling))
    sib.start()

    def load(i, carry):
        c_copy(chunk_of(i)).start()
        return carry

    lax.fori_loop(0, ring, load, 0)
    t_copy.start()

    def keep(block, h):
        high, low = split(near[block, :, h * part_depth:(h + 1) * part_depth].T)
        vt[h, block, :part_depth] = high
        vt[h, block, part_depth:] = low

    v_copy.wait()
    for h in range(HALVES):
        keep(col, h)
    sib.wait()
    for h in range(HALVES):
        keep(sibling, h)

    def arrive(h):
        for q in range(PIECES):
            y_copy(h, q).wait()
            forward(h, q).start()
        keep(across, h)
        for q in range(PIECES):
            forward(h, q).wait()
        keep(across_sibling, h)

    def job(i, h):
        chunk = chunk_of(i)
        total = None
        for b in range(blocks):
            high, low = split(c_ref[chunk, b * own:(b + 1) * own])
            both = jnp.dot(vt[h, b], high, preferred_element_type=F32)
            term = both[:part_depth] + (
                both[part_depth:] + jnp.dot(vt[h, b, :part_depth], low, preferred_element_type=F32)
            )
            total = term if total is None else total + term
        acc[chunk, h * part_depth:(h + 1) * part_depth] = total

    def first_job(i, carry):
        c_copy(chunk_of(i)).wait()
        job(i, 0)
        return carry

    def later_job(i, carry):
        job(i, 1)
        return carry

    part = part_depth // (2 * QUARTERS)

    def sum_send(h, way, step, q, src):
        rows = pl.ds(((h * 2 + way) * QUARTERS + q) * part, part)
        lane = h * 2 + way
        return remote(
            src.at[rows], got.at[step, rows], r_send.at[lane, step, q], r_recv.at[lane, step, q], (hops[way], col)
        )

    def begin(h):
        for q in range(QUARTERS):
            for way in range(2):
                sum_send(h, way, 0, q, acc.at[chunk_of(way)]).start()

    def reduce(h, step):
        for q in range(QUARTERS):
            for way in range(2):
                rows = pl.ds(((h * 2 + way) * QUARTERS + q) * part, part)
                chunk = wrap(at - 2 - step) if way == 0 else wrap(at + 2 + step)
                sum_send(h, way, step, q, got.at[step]).wait_recv()
                got[step, rows] += acc[chunk, rows]

                @pl.when(step < steps - 1)
                def _():
                    sum_send(h, way, step + 1, q, got.at[step]).start()

    arrive(0)
    lax.fori_loop(0, 2, first_job, 0)
    begin(0)
    lax.fori_loop(2, ring, first_job, 0)

    def early(t, carry):
        reduce(0, t)
        return carry

    def both_halves(t, carry):
        reduce(0, t)

        @pl.when(t >= LAG)
        def _():
            reduce(1, t - LAG)

        jobs = 2 * (t - LAG + 2)
        lax.fori_loop(jnp.minimum(jobs, ring), jnp.minimum(jobs + 2, ring), later_job, 0)
        return carry

    def late(t, carry):
        reduce(1, t - LAG)
        return carry

    lax.fori_loop(0, LAG - 1, early, 0)
    arrive(1)
    lax.fori_loop(0, 2, later_job, 0)
    begin(1)
    lax.fori_loop(LAG - 1, steps, both_halves, 0)
    t_copy.wait()
    t_high, t_low = split(t_ref[...])
    lax.fori_loop(steps, steps + LAG, late, 0)

    high, low = split(got[steps - 1])
    scaled[at] = dot3(t_high, t_low, high, low)
    g_part = depth // (2 * G_QUARTERS)

    def gather_send(way, step, q, chunk):
        ref = scaled.at[chunk, pl.ds((way * G_QUARTERS + q) * g_part, g_part)]
        return remote(ref, ref, g_send.at[way, step, q], g_recv.at[way, step, q], (hops[way], col))

    for q in range(G_QUARTERS):
        for way in range(2):
            gather_send(way, 0, q, at).start()

    def gather(step, carry):
        for q in range(G_QUARTERS):
            for way in range(2):
                chunk = wrap(at - 1 - step) if way == 0 else wrap(at + 1 + step)
                gather_send(way, step, q, chunk).wait_recv()

                @pl.when(step < steps - 1)
                def _():
                    gather_send(way, step + 1, q, chunk).start()

        return carry

    lax.fori_loop(0, steps, gather, 0)

    def sent(step, carry):
        for way in range(2):
            for h in range(HALVES):
                for q in range(QUARTERS):
                    sum_send(h, way, step, q, got.at[step]).wait_send()
            for q in range(G_QUARTERS):
                gather_send(way, step, q, at).wait_send()
        return carry

    lax.fori_loop(0, steps, sent, 0)


def update_kernel(c_ref, near, scaled, out_hbm, v_high, v_low, stage, sem):
    ring, height, width = c_ref.shape
    blocks, own, _ = near.shape
    for b in range(blocks):
        v_high[pl.ds(b * own, own)], v_low[pl.ds(b * own, own)] = split(near[b])
    slots = stage.shape[0]

    def out_copy(chunk, slot):
        return pltpu.make_async_copy(
            stage.at[slot], out_hbm.at[:, pl.ds(pl.multiple_of(chunk * width, width), width)], sem.at[slot]
        )

    def step(chunk, carry):
        slot = lax.rem(chunk, slots)

        @pl.when(chunk >= slots)
        def _():
            out_copy(chunk - slots, slot).wait()

        high, low = split(scaled[chunk])
        for b in range(blocks):
            rows = pl.ds(b * own, own)
            stage[slot, rows] = c_ref[chunk, rows] - dot3(v_high[rows], v_low[rows], high, low)
        out_copy(chunk, slot).start()
        return carry

    lax.fori_loop(0, ring, step, 0)
    for i in range(slots):
        chunk = ring - slots + i
        out_copy(chunk, chunk % slots).wait()


def ring_shards(ring, trailing, vectors, tfactor):
    height, columns = trailing.shape
    own, depth = vectors.shape
    width = columns // ring
    blocks = height // own
    steps = ring - 1
    dma = pltpu.SemaphoreType.DMA
    vmem = pl.BlockSpec(memory_space=pltpu.VMEM)
    hbm = pl.BlockSpec(memory_space=pl.ANY)
    held, near, scaled = pl.pallas_call(
        functools.partial(sum_kernel, ring),
        out_shape=(
            pltpu.VMEM((ring, height, width), F32),
            pltpu.VMEM((blocks, own, depth), F32),
            pltpu.VMEM((ring, depth, width), F32),
        ),
        in_specs=[hbm, hbm, hbm],
        out_specs=(vmem, vmem, vmem),
        scratch_shapes=[
            pltpu.VMEM((ring, depth, width), F32),
            pltpu.VMEM((HALVES, blocks, 2 * depth // HALVES, own), BF16),
            pltpu.VMEM((steps, depth, width), F32),
            pltpu.VMEM((depth, depth), F32),
            dma((ring,)), dma((2,)),
            dma, dma,
            dma((HALVES, PIECES)), dma((HALVES, PIECES)), dma((HALVES, PIECES)), dma((HALVES, PIECES)),
            dma((2 * HALVES, steps, QUARTERS)), dma((2 * HALVES, steps, QUARTERS)),
            dma((2, steps, G_QUARTERS)), dma((2, steps, G_QUARTERS)),
        ],
        compiler_params=pltpu.CompilerParams(
            collective_id=0, has_side_effects=True, vmem_limit_bytes=20 << 20
        ),
    )(trailing, vectors, tfactor)
    slots = min(4, ring)
    return pl.pallas_call(
        update_kernel,
        out_shape=jax.ShapeDtypeStruct((height, columns), F32),
        in_specs=[vmem, vmem, vmem],
        out_specs=hbm,
        scratch_shapes=[
            pltpu.VMEM((height, depth), BF16),
            pltpu.VMEM((height, depth), BF16),
            pltpu.VMEM((slots, height, width), F32),
            dma((slots,)),
        ],
        compiler_params=pltpu.CompilerParams(vmem_limit_bytes=20 << 20),
    )(held, near, scaled)


def plain_shards(trailing, vectors, tfactor):
    dot = functools.partial(jnp.dot, precision=lax.Precision.HIGH, preferred_element_type=F32)
    near_vectors = lax.all_gather(vectors, "col", axis=0, tiled=True)
    summed = lax.psum(dot(near_vectors.T, trailing), "row")
    return trailing - dot(near_vectors, dot(tfactor, summed))


def solution(mesh):
    ring, columns = mesh.shape["row"], mesh.shape["col"]
    placed = (P("row", "col"), P(("row", "col"), None), P())

    def shards(trailing, vectors, tfactor):
        width = trailing.shape[1] // ring
        if columns == 4 and ring % 2 == 0 and ring > 2 * LAG and width % 128 == 0:
            return ring_shards(ring, trailing, vectors, tfactor)
        return plain_shards(trailing, vectors, tfactor)

    return jax.shard_map(
        shards, mesh=mesh, in_specs=placed, out_specs=P("row", "col"), check_vma=False
    )
```

```python
import functools

import jax
import jax.numpy as jnp
from jax import lax
from jax.experimental import pallas as pl
from jax.experimental.pallas import tpu as pltpu
from jax.sharding import PartitionSpec as P

MESH = pl.DeviceIdType.MESH
F32, BF16 = jnp.float32, jnp.bfloat16
HALVES = 2
PIECES = 2
QUARTERS = 2
G_QUARTERS = 4
LAG = 2


def split(x):
    high = x.astype(BF16)
    return high, (x - high.astype(F32)).astype(BF16)


def dot3(a_high, a_low, b_high, b_low):
    dot = functools.partial(jnp.dot, preferred_element_type=F32)
    return dot(a_high, b_high) + (dot(a_low, b_high) + dot(a_high, b_low))


def sum_kernel(
    ring, c_hbm, v_hbm, t_hbm, c_ref, near, scaled,
    acc, vt, got, t_ref, c_sem, l_sem,
    sib_send, sib_recv, y_send, y_recv, f_send, f_recv, r_send, r_recv, g_send, g_recv,
):
    row, col = lax.axis_index("row"), lax.axis_index("col")
    core, y = lax.rem(col, 2), lax.div(col, 2)
    sibling = y * 2 + (1 - core)
    across = (1 - y) * 2 + core
    across_sibling = (1 - y) * 2 + (1 - core)
    half = ring // 2
    z, x = lax.div(row, 2), lax.rem(row, 2)
    at = jnp.where(x == 0, z, ring - 1 - z)

    def row_of(place):
        return jnp.where(place < half, 2 * place, 2 * (ring - 1 - place) + 1)

    def wrap(i):
        return lax.rem(i + 2 * ring, ring)

    hops = (row_of(wrap(at + 1)), row_of(wrap(at - 1)))
    blocks, own, depth = near.shape
    width = c_ref.shape[2]
    part_depth = depth // HALVES
    steps = ring - 1

    def chunk_of(i):
        step = lax.div(i, 2) + 1
        return jnp.where(i == ring - 1, at, wrap(jnp.where(lax.rem(i, 2) == 0, at - step, at + step)))

    def c_copy(chunk):
        return pltpu.make_async_copy(
            c_hbm.at[:, pl.ds(pl.multiple_of(chunk * width, width), width)], c_ref.at[chunk], c_sem.at[chunk]
        )

    v_copy = pltpu.make_async_copy(v_hbm, near.at[col], l_sem.at[0])
    t_copy = pltpu.make_async_copy(t_hbm, t_ref, l_sem.at[1])
    v_copy.start()

    barrier = pltpu.get_barrier_semaphore()
    friends = [(row, sibling), (row, across), (hops[0], col), (hops[1], col)]
    for friend in friends:
        pl.semaphore_signal(barrier, inc=1, device_id=friend, device_id_type=MESH)
    pl.semaphore_wait(barrier, len(friends))

    def remote(src, dst, send, recv, to):
        return pltpu.make_async_remote_copy(
            src_ref=src, dst_ref=dst, send_sem=send, recv_sem=recv, device_id=to, device_id_type=MESH
        )

    size = own // PIECES

    def y_copy(h, q):
        there = (pl.ds(q * size, size), pl.ds(h * part_depth, part_depth))
        return remote(near.at[(col,) + there], near.at[(col,) + there], y_send.at[h, q], y_recv.at[h, q], (row, across))

    def forward(h, q):
        there = (across, pl.ds(q * size, size), pl.ds(h * part_depth, part_depth))
        return remote(near.at[there], near.at[there], f_send.at[h, q], f_recv.at[h, q], (row, sibling))

    v_copy.wait()
    for h in range(HALVES):
        for q in range(PIECES):
            y_copy(h, q).start()
    sib = remote(near.at[col], near.at[col], sib_send, sib_recv, (row, sibling))
    sib.start()

    def load(i, carry):
        c_copy(chunk_of(i)).start()
        return carry

    lax.fori_loop(0, ring, load, 0)
    t_copy.start()

    def keep(block, h):
        high, low = split(near[block, :, h * part_depth:(h + 1) * part_depth].T)
        vt[h, block, :part_depth] = high
        vt[h, block, part_depth:] = low

    for h in range(HALVES):
        keep(col, h)
    sib.wait()
    for h in range(HALVES):
        keep(sibling, h)

    def arrive(h):
        for q in range(PIECES):
            y_copy(h, q).wait()
            forward(h, q).start()
        keep(across, h)
        for q in range(PIECES):
            forward(h, q).wait()
        keep(across_sibling, h)

    def product(h, block, high, low):
        both = jnp.dot(vt[h, block], high, preferred_element_type=F32)
        return both[:part_depth] + (
            both[part_depth:] + jnp.dot(vt[h, block, :part_depth], low, preferred_element_type=F32)
        )

    def pieces_of(chunk, pair):
        return [(b, split(c_ref[chunk, pl.ds(pl.multiple_of(b * own, own), own)])) for b in pair]

    def near_job(i, carry):
        chunk = chunk_of(i)
        c_copy(chunk).wait()
        (b0, c0), (b1, c1) = pieces_of(chunk, (col, sibling))
        for h in range(HALVES):
            acc[chunk, h * part_depth:(h + 1) * part_depth] = product(h, b0, *c0) + product(h, b1, *c1)
        return carry

    def job(i, h):
        chunk = chunk_of(i)
        (b0, c0), (b1, c1) = pieces_of(chunk, (across, across_sibling))
        acc[chunk, h * part_depth:(h + 1) * part_depth] += product(h, b0, *c0) + product(h, b1, *c1)

    def first_job(i, carry):
        job(i, 0)
        return carry

    def later_job(i, carry):
        job(i, 1)
        return carry

    part = part_depth // (2 * QUARTERS)

    def sum_send(h, way, step, q, src):
        rows = pl.ds(((h * 2 + way) * QUARTERS + q) * part, part)
        lane = h * 2 + way
        return remote(
            src.at[rows], got.at[step, rows], r_send.at[lane, step, q], r_recv.at[lane, step, q], (hops[way], col)
        )

    def begin(h):
        for q in range(QUARTERS):
            for way in range(2):
                sum_send(h, way, 0, q, acc.at[chunk_of(way)]).start()

    def reduce(h, step):
        for q in range(QUARTERS):
            for way in range(2):
                rows = pl.ds(((h * 2 + way) * QUARTERS + q) * part, part)
                chunk = wrap(at - 2 - step) if way == 0 else wrap(at + 2 + step)
                sum_send(h, way, step, q, got.at[step]).wait_recv()
                got[step, rows] += acc[chunk, rows]

                @pl.when(step < steps - 1)
                def _():
                    sum_send(h, way, step + 1, q, got.at[step]).start()

    lax.fori_loop(0, ring, near_job, 0)
    arrive(0)
    lax.fori_loop(0, 2, first_job, 0)
    begin(0)
    lax.fori_loop(2, ring, first_job, 0)

    def early(t, carry):
        reduce(0, t)
        return carry

    def both_halves(t, carry):
        reduce(0, t)

        @pl.when(t >= LAG)
        def _():
            reduce(1, t - LAG)

        jobs = 2 * (t - LAG + 2)
        lax.fori_loop(jnp.minimum(jobs, ring), jnp.minimum(jobs + 2, ring), later_job, 0)
        return carry

    def late(t, carry):
        reduce(1, t - LAG)
        return carry

    lax.fori_loop(0, LAG - 1, early, 0)
    arrive(1)
    lax.fori_loop(0, 2, later_job, 0)
    begin(1)
    lax.fori_loop(LAG - 1, steps, both_halves, 0)
    t_copy.wait()
    t_high, t_low = split(t_ref[...])
    lax.fori_loop(steps, steps + LAG, late, 0)

    high, low = split(got[steps - 1])
    scaled[at] = dot3(t_high, t_low, high, low)
    g_part = depth // (2 * G_QUARTERS)

    def gather_send(way, step, q, chunk):
        ref = scaled.at[chunk, pl.ds((way * G_QUARTERS + q) * g_part, g_part)]
        return remote(ref, ref, g_send.at[way, step, q], g_recv.at[way, step, q], (hops[way], col))

    for q in range(G_QUARTERS):
        for way in range(2):
            gather_send(way, 0, q, at).start()

    def gather(step, carry):
        for q in range(G_QUARTERS):
            for way in range(2):
                chunk = wrap(at - 1 - step) if way == 0 else wrap(at + 1 + step)
                gather_send(way, step, q, chunk).wait_recv()

                @pl.when(step < steps - 1)
                def _():
                    gather_send(way, step + 1, q, chunk).start()

        return carry

    lax.fori_loop(0, steps, gather, 0)

    def sent(step, carry):
        for way in range(2):
            for h in range(HALVES):
                for q in range(QUARTERS):
                    sum_send(h, way, step, q, got.at[step]).wait_send()
            for q in range(G_QUARTERS):
                gather_send(way, step, q, at).wait_send()
        return carry

    lax.fori_loop(0, steps, sent, 0)


def update_kernel(c_ref, near, scaled, out_hbm, v_high, v_low, stage, sem):
    ring, height, width = c_ref.shape
    blocks, own, _ = near.shape
    for b in range(blocks):
        v_high[pl.ds(b * own, own)], v_low[pl.ds(b * own, own)] = split(near[b])
    slots = stage.shape[0]

    def out_copy(chunk, slot):
        return pltpu.make_async_copy(
            stage.at[slot], out_hbm.at[:, pl.ds(pl.multiple_of(chunk * width, width), width)], sem.at[slot]
        )

    def step(chunk, carry):
        slot = lax.rem(chunk, slots)

        @pl.when(chunk >= slots)
        def _():
            out_copy(chunk - slots, slot).wait()

        high, low = split(scaled[chunk])
        for b in range(blocks):
            rows = pl.ds(b * own, own)
            stage[slot, rows] = c_ref[chunk, rows] - dot3(v_high[rows], v_low[rows], high, low)
        out_copy(chunk, slot).start()
        return carry

    lax.fori_loop(0, ring, step, 0)
    for i in range(slots):
        chunk = ring - slots + i
        out_copy(chunk, chunk % slots).wait()


def ring_shards(ring, trailing, vectors, tfactor):
    height, columns = trailing.shape
    own, depth = vectors.shape
    width = columns // ring
    blocks = height // own
    steps = ring - 1
    dma = pltpu.SemaphoreType.DMA
    vmem = pl.BlockSpec(memory_space=pltpu.VMEM)
    hbm = pl.BlockSpec(memory_space=pl.ANY)
    held, near, scaled = pl.pallas_call(
        functools.partial(sum_kernel, ring),
        out_shape=(
            pltpu.VMEM((ring, height, width), F32),
            pltpu.VMEM((blocks, own, depth), F32),
            pltpu.VMEM((ring, depth, width), F32),
        ),
        in_specs=[hbm, hbm, hbm],
        out_specs=(vmem, vmem, vmem),
        scratch_shapes=[
            pltpu.VMEM((ring, depth, width), F32),
            pltpu.VMEM((HALVES, blocks, 2 * depth // HALVES, own), BF16),
            pltpu.VMEM((steps, depth, width), F32),
            pltpu.VMEM((depth, depth), F32),
            dma((ring,)), dma((2,)),
            dma, dma,
            dma((HALVES, PIECES)), dma((HALVES, PIECES)), dma((HALVES, PIECES)), dma((HALVES, PIECES)),
            dma((2 * HALVES, steps, QUARTERS)), dma((2 * HALVES, steps, QUARTERS)),
            dma((2, steps, G_QUARTERS)), dma((2, steps, G_QUARTERS)),
        ],
        compiler_params=pltpu.CompilerParams(
            collective_id=0, has_side_effects=True, vmem_limit_bytes=20 << 20
        ),
    )(trailing, vectors, tfactor)
    slots = min(4, ring)
    return pl.pallas_call(
        update_kernel,
        out_shape=jax.ShapeDtypeStruct((height, columns), F32),
        in_specs=[vmem, vmem, vmem],
        out_specs=hbm,
        scratch_shapes=[
            pltpu.VMEM((height, depth), BF16),
            pltpu.VMEM((height, depth), BF16),
            pltpu.VMEM((slots, height, width), F32),
            dma((slots,)),
        ],
        compiler_params=pltpu.CompilerParams(vmem_limit_bytes=20 << 20),
    )(held, near, scaled)


def plain_shards(trailing, vectors, tfactor):
    dot = functools.partial(jnp.dot, precision=lax.Precision.HIGH, preferred_element_type=F32)
    near_vectors = lax.all_gather(vectors, "col", axis=0, tiled=True)
    summed = lax.psum(dot(near_vectors.T, trailing), "row")
    return trailing - dot(near_vectors, dot(tfactor, summed))


def solution(mesh):
    ring, columns = mesh.shape["row"], mesh.shape["col"]
    placed = (P("row", "col"), P(("row", "col"), None), P())

    def shards(trailing, vectors, tfactor):
        width = trailing.shape[1] // ring
        if columns == 4 and ring % 2 == 0 and ring > 2 * LAG and width % 128 == 0:
            return ring_shards(ring, trailing, vectors, tfactor)
        return plain_shards(trailing, vectors, tfactor)

    return jax.shard_map(
        shards, mesh=mesh, in_specs=placed, out_specs=P("row", "col"), check_vma=False
    )
```

```python
import functools

import jax
import jax.numpy as jnp
from jax import lax
from jax.experimental import pallas as pl
from jax.experimental.pallas import tpu as pltpu
from jax.sharding import PartitionSpec as P

MESH = pl.DeviceIdType.MESH
F32, BF16 = jnp.float32, jnp.bfloat16
HALVES = 2
PIECES = 4
QUARTERS = 2
G_QUARTERS = 8
LAG = 2


def split(x):
    high = x.astype(BF16)
    return high, (x - high.astype(F32)).astype(BF16)


def dot3(a_high, a_low, b_high, b_low):
    dot = functools.partial(jnp.dot, preferred_element_type=F32)
    return dot(a_high, b_high) + (dot(a_low, b_high) + dot(a_high, b_low))


def sum_kernel(
    ring, c_hbm, v_hbm, t_hbm, c_ref, near, scaled,
    acc, vt, got, t_ref, c_sem, l_sem,
    sib_send, sib_recv, y_send, y_recv, f_send, f_recv, r_send, r_recv, g_send, g_recv,
):
    row, col = lax.axis_index("row"), lax.axis_index("col")
    core, y = lax.rem(col, 2), lax.div(col, 2)
    sibling = y * 2 + (1 - core)
    across = (1 - y) * 2 + core
    across_sibling = (1 - y) * 2 + (1 - core)
    half = ring // 2
    z, x = lax.div(row, 2), lax.rem(row, 2)
    at = jnp.where(x == 0, z, ring - 1 - z)

    def row_of(place):
        return jnp.where(place < half, 2 * place, 2 * (ring - 1 - place) + 1)

    def wrap(i):
        return lax.rem(i + 2 * ring, ring)

    hops = (row_of(wrap(at + 1)), row_of(wrap(at - 1)))
    blocks, own, depth = near.shape
    width = c_ref.shape[2]
    part_depth = depth // HALVES
    steps = ring - 1

    def chunk_of(i):
        step = lax.div(i, 2) + 1
        return jnp.where(i == ring - 1, at, wrap(jnp.where(lax.rem(i, 2) == 0, at - step, at + step)))

    def c_copy(chunk):
        return pltpu.make_async_copy(
            c_hbm.at[:, pl.ds(pl.multiple_of(chunk * width, width), width)], c_ref.at[chunk], c_sem.at[chunk]
        )

    v_copy = pltpu.make_async_copy(v_hbm, near.at[col], l_sem.at[0])
    t_copy = pltpu.make_async_copy(t_hbm, t_ref, l_sem.at[1])
    v_copy.start()

    barrier = pltpu.get_barrier_semaphore()
    friends = [(row, sibling), (row, across), (hops[0], col), (hops[1], col)]
    for friend in friends:
        pl.semaphore_signal(barrier, inc=1, device_id=friend, device_id_type=MESH)
    pl.semaphore_wait(barrier, len(friends))

    def remote(src, dst, send, recv, to):
        return pltpu.make_async_remote_copy(
            src_ref=src, dst_ref=dst, send_sem=send, recv_sem=recv, device_id=to, device_id_type=MESH
        )

    size = own // PIECES

    def y_copy(h, q):
        there = (pl.ds(q * size, size), pl.ds(h * part_depth, part_depth))
        return remote(near.at[(col,) + there], near.at[(col,) + there], y_send.at[h, q], y_recv.at[h, q], (row, across))

    def forward(h, q):
        there = (across, pl.ds(q * size, size), pl.ds(h * part_depth, part_depth))
        return remote(near.at[there], near.at[there], f_send.at[h, q], f_recv.at[h, q], (row, sibling))

    v_copy.wait()
    for h in range(HALVES):
        for q in range(PIECES):
            y_copy(h, q).start()
    sib = remote(near.at[col], near.at[col], sib_send, sib_recv, (row, sibling))
    sib.start()

    def load(i, carry):
        c_copy(chunk_of(i)).start()
        return carry

    lax.fori_loop(0, ring, load, 0)
    t_copy.start()

    def keep(block, h):
        high, low = split(near[block, :, h * part_depth:(h + 1) * part_depth].T)
        vt[h, block, :part_depth] = high
        vt[h, block, part_depth:] = low

    for h in range(HALVES):
        keep(col, h)
    sib.wait()
    for h in range(HALVES):
        keep(sibling, h)

    def arrive(h):
        for q in range(PIECES):
            y_copy(h, q).wait()
            forward(h, q).start()
        keep(across, h)
        for q in range(PIECES):
            forward(h, q).wait()
        keep(across_sibling, h)

    def product(h, block, high, low):
        both = jnp.dot(vt[h, block], high, preferred_element_type=F32)
        return both[:part_depth] + (
            both[part_depth:] + jnp.dot(vt[h, block, :part_depth], low, preferred_element_type=F32)
        )

    def pieces_of(chunk, pair):
        return [(b, split(c_ref[chunk, pl.ds(pl.multiple_of(b * own, own), own)])) for b in pair]

    def near_job(i, carry):
        chunk = chunk_of(i)
        c_copy(chunk).wait()
        (b0, c0), (b1, c1) = pieces_of(chunk, (col, sibling))
        for h in range(HALVES):
            acc[chunk, h * part_depth:(h + 1) * part_depth] = product(h, b0, *c0) + product(h, b1, *c1)
        return carry

    def job(i, h):
        chunk = chunk_of(i)
        (b0, c0), (b1, c1) = pieces_of(chunk, (across, across_sibling))
        acc[chunk, h * part_depth:(h + 1) * part_depth] += product(h, b0, *c0) + product(h, b1, *c1)

    def first_job(i, carry):
        job(i, 0)
        return carry

    def later_job(i, carry):
        job(i, 1)
        return carry

    part = part_depth // (2 * QUARTERS)

    def sum_send(h, way, step, q, src):
        rows = pl.ds(((h * 2 + way) * QUARTERS + q) * part, part)
        lane = h * 2 + way
        return remote(
            src.at[rows], got.at[step, rows], r_send.at[lane, step, q], r_recv.at[lane, step, q], (hops[way], col)
        )

    def begin(h):
        for q in range(QUARTERS):
            for way in range(2):
                sum_send(h, way, 0, q, acc.at[chunk_of(way)]).start()

    def reduce(h, step):
        for q in range(QUARTERS):
            for way in range(2):
                rows = pl.ds(((h * 2 + way) * QUARTERS + q) * part, part)
                chunk = wrap(at - 2 - step) if way == 0 else wrap(at + 2 + step)
                sum_send(h, way, step, q, got.at[step]).wait_recv()
                got[step, rows] += acc[chunk, rows]

                @pl.when(step < steps - 1)
                def _():
                    sum_send(h, way, step + 1, q, got.at[step]).start()

    lax.fori_loop(0, ring, near_job, 0)
    arrive(0)
    lax.fori_loop(0, 2, first_job, 0)
    begin(0)
    lax.fori_loop(2, ring, first_job, 0)

    def early(t, carry):
        reduce(0, t)
        return carry

    def both_halves(t, carry):
        reduce(0, t)

        @pl.when(t >= LAG)
        def _():
            reduce(1, t - LAG)

        jobs = 2 * (t - LAG + 2)
        lax.fori_loop(jnp.minimum(jobs, ring), jnp.minimum(jobs + 2, ring), later_job, 0)
        return carry

    def late(t, carry):
        reduce(1, t - LAG)
        return carry

    lax.fori_loop(0, LAG - 1, early, 0)
    arrive(1)
    lax.fori_loop(0, 2, later_job, 0)
    begin(1)
    lax.fori_loop(LAG - 1, steps, both_halves, 0)
    t_copy.wait()
    t_high, t_low = split(t_ref[...])
    lax.fori_loop(steps, steps + LAG, late, 0)

    high, low = split(got[steps - 1])
    scaled[at] = dot3(t_high, t_low, high, low)
    g_part = depth // (2 * G_QUARTERS)

    def gather_send(way, step, q, chunk):
        ref = scaled.at[chunk, pl.ds((way * G_QUARTERS + q) * g_part, g_part)]
        return remote(ref, ref, g_send.at[way, step, q], g_recv.at[way, step, q], (hops[way], col))

    for q in range(G_QUARTERS):
        for way in range(2):
            gather_send(way, 0, q, at).start()

    def gather(step, carry):
        for q in range(G_QUARTERS):
            for way in range(2):
                chunk = wrap(at - 1 - step) if way == 0 else wrap(at + 1 + step)
                gather_send(way, step, q, chunk).wait_recv()

                @pl.when(step < steps - 1)
                def _():
                    gather_send(way, step + 1, q, chunk).start()

        return carry

    lax.fori_loop(0, steps, gather, 0)

    def sent(step, carry):
        for way in range(2):
            for h in range(HALVES):
                for q in range(QUARTERS):
                    sum_send(h, way, step, q, got.at[step]).wait_send()
            for q in range(G_QUARTERS):
                gather_send(way, step, q, at).wait_send()
        return carry

    lax.fori_loop(0, steps, sent, 0)


def update_kernel(c_ref, near, scaled, out_hbm, v_high, v_low, stage, sem):
    ring, height, width = c_ref.shape
    blocks, own, _ = near.shape
    for b in range(blocks):
        v_high[pl.ds(b * own, own)], v_low[pl.ds(b * own, own)] = split(near[b])
    slots = stage.shape[0]

    def out_copy(chunk, slot):
        return pltpu.make_async_copy(
            stage.at[slot], out_hbm.at[:, pl.ds(pl.multiple_of(chunk * width, width), width)], sem.at[slot]
        )

    def step(chunk, carry):
        slot = lax.rem(chunk, slots)

        @pl.when(chunk >= slots)
        def _():
            out_copy(chunk - slots, slot).wait()

        high, low = split(scaled[chunk])
        for b in range(blocks):
            rows = pl.ds(b * own, own)
            stage[slot, rows] = c_ref[chunk, rows] - dot3(v_high[rows], v_low[rows], high, low)
        out_copy(chunk, slot).start()
        return carry

    lax.fori_loop(0, ring, step, 0)
    for i in range(slots):
        chunk = ring - slots + i
        out_copy(chunk, chunk % slots).wait()


def ring_shards(ring, trailing, vectors, tfactor):
    height, columns = trailing.shape
    own, depth = vectors.shape
    width = columns // ring
    blocks = height // own
    steps = ring - 1
    dma = pltpu.SemaphoreType.DMA
    vmem = pl.BlockSpec(memory_space=pltpu.VMEM)
    hbm = pl.BlockSpec(memory_space=pl.ANY)
    held, near, scaled = pl.pallas_call(
        functools.partial(sum_kernel, ring),
        out_shape=(
            pltpu.VMEM((ring, height, width), F32),
            pltpu.VMEM((blocks, own, depth), F32),
            pltpu.VMEM((ring, depth, width), F32),
        ),
        in_specs=[hbm, hbm, hbm],
        out_specs=(vmem, vmem, vmem),
        scratch_shapes=[
            pltpu.VMEM((ring, depth, width), F32),
            pltpu.VMEM((HALVES, blocks, 2 * depth // HALVES, own), BF16),
            pltpu.VMEM((steps, depth, width), F32),
            pltpu.VMEM((depth, depth), F32),
            dma((ring,)), dma((2,)),
            dma, dma,
            dma((HALVES, PIECES)), dma((HALVES, PIECES)), dma((HALVES, PIECES)), dma((HALVES, PIECES)),
            dma((2 * HALVES, steps, QUARTERS)), dma((2 * HALVES, steps, QUARTERS)),
            dma((2, steps, G_QUARTERS)), dma((2, steps, G_QUARTERS)),
        ],
        compiler_params=pltpu.CompilerParams(
            collective_id=0, has_side_effects=True, vmem_limit_bytes=20 << 20
        ),
    )(trailing, vectors, tfactor)
    slots = min(4, ring)
    return pl.pallas_call(
        update_kernel,
        out_shape=jax.ShapeDtypeStruct((height, columns), F32),
        in_specs=[vmem, vmem, vmem],
        out_specs=hbm,
        scratch_shapes=[
            pltpu.VMEM((height, depth), BF16),
            pltpu.VMEM((height, depth), BF16),
            pltpu.VMEM((slots, height, width), F32),
            dma((slots,)),
        ],
        compiler_params=pltpu.CompilerParams(vmem_limit_bytes=20 << 20),
    )(held, near, scaled)


def plain_shards(trailing, vectors, tfactor):
    dot = functools.partial(jnp.dot, precision=lax.Precision.HIGH, preferred_element_type=F32)
    near_vectors = lax.all_gather(vectors, "col", axis=0, tiled=True)
    summed = lax.psum(dot(near_vectors.T, trailing), "row")
    return trailing - dot(near_vectors, dot(tfactor, summed))


def solution(mesh):
    ring, columns = mesh.shape["row"], mesh.shape["col"]
    placed = (P("row", "col"), P(("row", "col"), None), P())

    def shards(trailing, vectors, tfactor):
        width = trailing.shape[1] // ring
        if columns == 4 and ring % 2 == 0 and ring > 2 * LAG and width % 128 == 0:
            return ring_shards(ring, trailing, vectors, tfactor)
        return plain_shards(trailing, vectors, tfactor)

    return jax.shard_map(
        shards, mesh=mesh, in_specs=placed, out_specs=P("row", "col"), check_vma=False
    )
```
